32 devices in a mesh: px: 16 (over z, x, core), py: 2 (over y).
Axes of the slice: x: 2, y: 2, z: 4, core: 2. Of those that a mesh axis runs over, the one named last changes fastest.
Arguments:
- velocity: float32 [3, 1024, 2, 1024], P(None, 'px', 'py'), may hold values from -1.5 to 2.5
- band_of: int32 [2], replicated, may hold values from 0 to 1, as said below
Outputs:
- correlation: float32 [6, 2, 1024, 1024], P(None, None, ('px', 'py'))
The draws below stay inside these ranges and needn't reach their ends.
Inputs may be any that keep to these rules, and one draw needn't show every extreme that they name: `band_of`: every band 0 to 1 holds at least one plane.
All inputs are finite; a program needn't handle non-finite values.
Results may differ from the reference program's by a relative error of at most 0.00013.
Values sent between devices are 32-bit elements; how exact they have to be, the bound alone decides.
A program may use at most 64 MiB of HBM per device.

```python
import math
import jax
import jax.numpy as jnp
from jax import lax

NX = 1024
NZ = 1024
NY = 2
NB = 2


def draw_band_of(key, part):
    first_key = jax.random.fold_in(key, 11)
    second_key = jax.random.fold_in(key, 23)
    random_band = jax.random.randint(first_key, (NY,), 0, NB, dtype=jnp.int32)
    shuffled = jax.random.permutation(second_key, jnp.arange(NY, dtype=jnp.int32))
    return jnp.where(shuffled < NB, shuffled, random_band).astype(jnp.int32)


def level_of(key, dims, cuts, low, high):
    level, own = 1.0, jax.random.fold_in(key, 6)
    for axis_at, blocks in cuts:
        draws = jnp.exp(jax.random.uniform(jax.random.fold_in(own, axis_at), (blocks,), jnp.float32, low / len(cuts), high / len(cuts)))
        level = level * jnp.repeat(draws, dims[axis_at] // blocks).reshape([-1 if axis == axis_at else 1 for axis in range(len(dims))])
    return level


def setup_inputs(seed: int = 0) -> dict:
    splits = jax.random.split(jax.random.key(seed), 3)
    velocity = jnp.clip(-1.5 + 4.0 * jax.random.uniform(splits[0], (3, NX, NY, NZ), jnp.float32) ** level_of(splits[0], (3, NX, NY, NZ), ((1, 16), (2, 2)), -0.2, 0.2), -1.5, 2.5)
    band_of = draw_band_of(jax.random.fold_in(splits[2], 71), 0)
    return dict(velocity=velocity, band_of=band_of)


PAIR_LIST = ((0, 0), (0, 1), (0, 2), (1, 1), (1, 2), (2, 2))

def reference(velocity, band_of):
    half = NZ // 2
    cells = NX * NZ
    span_spec = jnp.fft.rfft(velocity, axis=3)[..., :half]
    spectrum = jnp.fft.fft(span_spec, axis=1)
    spectrum = spectrum.at[:, 0, :, 0].set(0.0)
    band_ids = jnp.arange(NB, dtype=jnp.int32)
    onehot = (band_of[:, None] == band_ids[None, :]).astype(jnp.float32)
    counts = lax.optimization_barrier(jnp.sum(onehot, 0))
    band_weight = onehot / (counts[None, :] * (cells * math.sqrt(cells)))
    results = []
    for left_comp, right_comp in PAIR_LIST:
        product = jnp.conj(spectrum[left_comp]) * spectrum[right_comp]
        banded_real = jnp.einsum('xyk,yb->bxk', jnp.real(product), band_weight, precision=lax.Precision.HIGHEST)
        banded_imag = jnp.einsum('xyk,yb->bxk', jnp.imag(product), band_weight, precision=lax.Precision.HIGHEST)
        stream_back = jnp.fft.ifft(lax.complex(banded_real, banded_imag), axis=1) * NX
        padded = jnp.concatenate((stream_back, jnp.zeros((NB, NX, 1), stream_back.dtype)), 2)
        results.append(jnp.fft.irfft(padded, n=NZ, axis=2) * NZ)
    return jnp.stack(results, 0)
```

```python
import functools
import math

import jax
import jax.numpy as jnp
import numpy as np
from jax import lax
from jax.experimental import pallas as pl
from jax.experimental.pallas import tpu as pltpu
from jax.sharding import PartitionSpec as P

NB = 2


PAIR_LIST = ((0, 0), (0, 1), (0, 2), (1, 1), (1, 2), (2, 2))


def phase_table(row_values, offset, count, length):
    col_values = offset + lax.iota(jnp.int32, count)
    phase = row_values[:, None] * col_values[None, :] % length
    angle = phase.astype(jnp.float32) * (2.0 * math.pi / length)
    return (jnp.cos(angle), jnp.sin(angle))


def transform_last(real_part, imag_part, sign):
    full_shape = real_part.shape
    length = full_shape[-1]
    stacked = jnp.concatenate((real_part.reshape(-1, length), imag_part.reshape(-1, length)), 0)
    row_count = stacked.shape[0] // 2
    row_values = lax.iota(jnp.int32, length)

    def one_block(block_index, outputs):
        offset = (block_index * 128).astype(jnp.int32)
        cosine_table, sine_table = phase_table(row_values, offset, 128, length)
        with_cos = jnp.dot(
            stacked,
            cosine_table,
            precision=lax.Precision.HIGHEST,
            preferred_element_type=jnp.float32,
        )
        with_sin = jnp.dot(
            stacked, sine_table, precision=lax.Precision.HIGHEST, preferred_element_type=jnp.float32
        )
        new_real = with_cos[:row_count] - sign * with_sin[row_count:]
        new_imag = with_cos[row_count:] + sign * with_sin[:row_count]
        return (
            lax.dynamic_update_slice_in_dim(outputs[0], new_real, offset, 1),
            lax.dynamic_update_slice_in_dim(outputs[1], new_imag, offset, 1),
        )

    zeros = jnp.zeros((row_count, length), jnp.float32)
    out_real, out_imag = lax.fori_loop(0, length // 128, one_block, (zeros, zeros))
    return (out_real.reshape(full_shape), out_imag.reshape(full_shape))


def span_forward(velocity):
    comps, rows_x, planes, length = velocity.shape
    half = length // 2
    row_values = lax.iota(jnp.int32, length)

    def one_block(block_index, outputs):
        offset = (block_index * 128).astype(jnp.int32)
        cosine_table, sine_table = phase_table(row_values, offset, 128, length)
        with_cos = jnp.einsum(
            "cxpz,zk->cpkx",
            velocity,
            cosine_table,
            precision=lax.Precision.HIGHEST,
            preferred_element_type=jnp.float32,
        )
        with_sin = jnp.einsum(
            "cxpz,zk->cpkx",
            velocity,
            sine_table,
            precision=lax.Precision.HIGHEST,
            preferred_element_type=jnp.float32,
        )
        return (
            lax.dynamic_update_slice_in_dim(outputs[0], with_cos, offset, 2),
            lax.dynamic_update_slice_in_dim(outputs[1], -with_sin, offset, 2),
        )

    zeros = jnp.zeros((comps, planes, half, rows_x), jnp.float32)
    return lax.fori_loop(0, half // 128, one_block, (zeros, zeros))


def span_inverse(summed, kz_order):
    half = summed.shape[3]
    length = 2 * half
    multiplier = jnp.where(kz_order == 0, 1.0, 2.0).astype(jnp.float32)
    held_real = summed[:, :, 0] * multiplier[:, None]
    held_imag = summed[:, :, 1] * multiplier[:, None]

    def one_block(block_index, output):
        offset = (block_index * 128).astype(jnp.int32)
        cosine_table, sine_table = phase_table(kz_order, offset, 128, length)
        part = jnp.einsum(
            "sbkd,kz->sbdz",
            held_real,
            cosine_table,
            precision=lax.Precision.HIGHEST,
            preferred_element_type=jnp.float32,
        )
        part = part - jnp.einsum(
            "sbkd,kz->sbdz",
            held_imag,
            sine_table,
            precision=lax.Precision.HIGHEST,
            preferred_element_type=jnp.float32,
        )
        return lax.dynamic_update_slice_in_dim(output, part, offset, 3)

    zeros = jnp.zeros((summed.shape[0], summed.shape[1], summed.shape[4], length), jnp.float32)
    return lax.fori_loop(0, length // 128, one_block, zeros)


def general_device(velocity, band_of):
    px_count = lax.axis_size("px")
    py_count = lax.axis_size("py")
    comps, rows_x, planes, span = velocity.shape
    stream = rows_x * px_count
    half = span // 2
    local_k = half // px_count
    span_real, span_imag = span_forward(velocity)
    planes_spec = jnp.stack((span_real, span_imag), 1)
    kz_index = lax.iota(jnp.int32, local_k)
    kx_index = lax.iota(jnp.int32, stream)
    at_anchor = jnp.logical_and(
        lax.axis_index("px") == 0, jnp.logical_and(kz_index[:, None] == 0, kx_index[None, :] == 0)
    )
    keep_mask = 1.0 - at_anchor.astype(jnp.float32)
    received = lax.all_to_all(planes_spec, "px", split_axis=3, concat_axis=4, tiled=True)
    front_real, front_imag = transform_last(received[:, 0], received[:, 1], -1.0)
    spectrum = jnp.stack((front_real * keep_mask, front_imag * keep_mask), 1)
    cross_list = []
    for left_comp, right_comp in PAIR_LIST:
        left_real, left_imag = (spectrum[left_comp, 0], spectrum[left_comp, 1])
        right_real, right_imag = (spectrum[right_comp, 0], spectrum[right_comp, 1])
        cross_list.append(
            jnp.stack(
                (
                    left_real * right_real + left_imag * right_imag,
                    left_real * right_imag - left_imag * right_real,
                ),
                0,
            )
        )
    cross = jnp.stack(cross_list, 0)
    band_ids = lax.iota(jnp.int32, NB)
    onehot_all = (band_of[:, None] == band_ids[None, :]).astype(jnp.float32)
    counts = jnp.sum(onehot_all, 0)
    cells = float(stream * span)
    plane_start = lax.axis_index("py") * planes
    local_hot = lax.dynamic_slice_in_dim(onehot_all, plane_start, planes, 0)
    band_weight = local_hot / (counts[None, :] * (cells * math.sqrt(cells)))
    banded = jnp.einsum("sapkx,pb->sbakx", cross, band_weight, precision=lax.Precision.HIGHEST)
    summed = lax.psum_scatter(banded, "py", scatter_dimension=3, tiled=True)
    back_real, back_imag = transform_last(summed[:, :, 0], summed[:, :, 1], 1.0)
    exchanged = lax.all_to_all(
        lax.all_to_all(
            jnp.stack((back_real, back_imag), 2), "px", split_axis=4, concat_axis=3, tiled=True
        ),
        "py",
        split_axis=4,
        concat_axis=3,
        tiled=True,
    )
    quarter = local_k // py_count
    position = lax.iota(jnp.int32, half)
    outer = position // (px_count * quarter)
    remain = position % (px_count * quarter)
    kz_order = remain // quarter * local_k + outer * quarter + remain % quarter
    return span_inverse(exchanged, kz_order)


def split_table(table):
    high = table.astype(jnp.bfloat16)
    low = (table - high.astype(np.float64)).astype(jnp.bfloat16)
    return high, low


def span_tables(length):
    quarter, eighth = length // 4, length // 8
    column = np.arange(quarter)

    def angle(first, count):
        wave = 4 * np.arange(count) + first
        return 2.0 * np.pi * ((wave[:, None] * column[None, :]) % length) / length

    even = angle(0, eighth)
    middle = angle(2, eighth)
    odd = angle(1, quarter)
    table_even = np.concatenate((np.cos(even), -np.sin(even)), 0)
    table_middle = np.concatenate((np.cos(middle), -np.sin(middle)), 0)
    table_odd = np.block([[np.cos(odd), -np.sin(odd)], [-np.sin(odd), -np.cos(odd)]])
    return split_table(table_even) + split_table(table_middle) + split_table(table_odd)


def stream_tables(length):
    quarter = length // 4
    index = np.arange(quarter)
    angle = 2.0 * np.pi * ((index[:, None] * index[None, :]) % quarter) / quarter
    cosine, sine = np.cos(angle), np.sin(angle)
    twist = 2.0 * np.pi * (np.arange(4)[:, None] * index[None, :]) / length
    twiddle = np.concatenate((np.cos(twist), np.sin(twist)), 0).astype(np.float32)
    return split_table(np.block([[cosine, -sine], [sine, cosine]])) + (twiddle,)


def split_value(value):
    high = value.astype(jnp.bfloat16)
    low = (value - high.astype(jnp.float32)).astype(jnp.bfloat16)
    return high, low


def three_dots(left, right, dims):
    def one(a, b):
        return lax.dot_general(a, b, (dims, ((), ())), preferred_element_type=jnp.float32)

    return one(left[0], right[0]) + (one(left[1], right[0]) + one(left[0], right[1]))


NT = ((1,), (1,))
NN = ((1,), (0,))


def span_kernel(share, v_ref, e_h, e_l, m_h, m_l, o_h, o_l, out_ref):
    values = v_ref[...]
    rows = values.shape[0] // 3
    values = jnp.concatenate((values, values[2 * rows :]), 0)
    quarter = values.shape[1] // 4
    part = [values[:, i * quarter : (i + 1) * quarter] for i in range(4)]
    plus_even, plus_odd = part[0] + part[2], part[1] + part[3]
    odd_in = jnp.concatenate((part[0] - part[2], part[1] - part[3]), 1)
    even = three_dots((e_h[...], e_l[...]), split_value(plus_even + plus_odd), NT)
    middle = three_dots((m_h[...], m_l[...]), split_value(plus_even - plus_odd), NT)
    odd = three_dots((o_h[...], o_l[...]), split_value(odd_in), NT)
    eighth = quarter // 2
    real = jnp.concatenate((even[:eighth], middle[:eighth], odd[:quarter]), 0)
    imag = jnp.concatenate((even[eighth:], middle[eighth:], odd[quarter:]), 0)
    lane = lax.broadcasted_iota(jnp.int32, (real.shape[0], 128), 1)
    third = jnp.where(lane < 64, real[:, 128:], imag[:, 128:])
    out_ref[:, :share] = real[:, :128].reshape(-1, share, 128)
    out_ref[:, share : 2 * share] = imag[:, :128].reshape(-1, share, 128)
    out_ref[:, 2 * share :] = third.reshape(-1, share, 128)


def stream_kernel(share, planes, me_ref, weight_ref, in_ref, t_h, t_l, w_ref, out_ref):
    first_device = me_ref[0] == 0
    px_count = in_ref.shape[0] // planes
    columns = px_count // 2
    group_cols = columns // 4
    quarter = w_ref.shape[1]
    lane = lax.broadcasted_iota(jnp.int32, (3 * share, 128), 1)
    low_half = lane < 64
    cells = []
    for q in range(columns):
        real, imag = [[], [], []], [[], [], []]
        for y in range(planes):
            a = in_ref[2 * q * planes + y]
            b = in_ref[(2 * q + 1) * planes + y]
            low = jnp.where(low_half, a, pltpu.roll(b, 64, 1))
            high = jnp.where(low_half, pltpu.roll(a, 64, 1), b)
            real[0].append(low[:share])
            imag[0].append(low[share : 2 * share])
            real[1].append(high[:share])
            imag[1].append(high[share : 2 * share])
            real[2].append(low[2 * share :])
            imag[2].append(high[2 * share :])
        cells.append(
            (
                jnp.concatenate(real[0] + real[1] + real[2], 0),
                jnp.concatenate(imag[0] + imag[1] + imag[2], 0),
            )
        )
    part = [
        tuple(
            jnp.concatenate([cells[j * group_cols + g][ri] for g in range(group_cols)], 1)
            for ri in range(2)
        )
        for j in range(4)
    ]
    sum02 = [part[0][i] + part[2][i] for i in range(2)]
    dif02 = [part[0][i] - part[2][i] for i in range(2)]
    sum13 = [part[1][i] + part[3][i] for i in range(2)]
    dif13 = [part[1][i] - part[3][i] for i in range(2)]
    mixed = [
        (sum02[0] + sum13[0], sum02[1] + sum13[1]),
        (dif02[0] + dif13[1], dif02[1] - dif13[0]),
        (sum02[0] - sum13[0], sum02[1] - sum13[1]),
        (dif02[0] - dif13[1], dif02[1] + dif13[0]),
    ]
    turned = []
    for k1, (real, imag) in enumerate(mixed):
        if k1:
            cosine, sine = w_ref[k1 : k1 + 1], w_ref[4 + k1 : 5 + k1]
            real, imag = real * cosine + imag * sine, imag * cosine - real * sine
        turned.append(jnp.concatenate((real, imag), 1))
    table = (t_h[...], t_l[...])
    front = three_dots(split_value(jnp.concatenate(turned, 0)), table, NN)
    block = 3 * planes * share
    row = lax.broadcasted_iota(jnp.int32, (block, 2 * quarter), 0)
    col = lax.broadcasted_iota(jnp.int32, (block, 2 * quarter), 1)
    anchor = jnp.logical_and(row % share == 0, col % quarter == 0)
    anchor = jnp.logical_and(anchor, first_device)
    front = jnp.concatenate((jnp.where(anchor, 0.0, front[:block]), front[block:]), 0)
    front = front.reshape(4, 3, planes, share, 2 * quarter)
    field = [
        [
            (
                front[:, c, y, :, :quarter].reshape(4 * share, quarter),
                front[:, c, y, :, quarter:].reshape(4 * share, quarter),
            )
            for y in range(planes)
        ]
        for c in range(3)
    ]
    row = lax.broadcasted_iota(jnp.int32, (4 * share, quarter), 0)
    single = jnp.logical_and(row % share == 0, first_device)
    multiplier = jnp.where(single, 1.0, 2.0)
    own, mutual = [], []
    for left, right in PAIR_LIST:
        real_sum, imag_sum = [None] * NB, [None] * NB
        for y in range(planes):
            lr, li = field[left][y]
            rr, ri = field[right][y]
            real = lr * rr + li * ri
            imag = None if left == right else lr * ri - li * rr
            for b in range(NB):
                weight = weight_ref[y * NB + b]
                add = weight * real
                real_sum[b] = add if y == 0 else real_sum[b] + add
                if imag is not None:
                    add = weight * imag
                    imag_sum[b] = add if y == 0 else imag_sum[b] + add
        for b in range(NB):
            if left == right:
                own.append(real_sum[b] * multiplier)
            else:
                mutual.append(
                    jnp.concatenate((real_sum[b] * multiplier, imag_sum[b] * multiplier), 1)
                )
    own_table = (t_h[:, :quarter], t_l[:, :quarter])
    own_back = three_dots(split_value(jnp.concatenate(own, 0)), own_table, NT)
    mutual_back = three_dots(split_value(jnp.concatenate(mutual, 0)), table, NT)
    lines = []
    own_at = mutual_at = 0
    for left, right in PAIR_LIST:
        for b in range(NB):
            if left == right:
                back = own_back[own_at * 4 * share : (own_at + 1) * 4 * share]
                own_at += 1
            else:
                back = mutual_back[mutual_at * 4 * share : (mutual_at + 1) * 4 * share]
                mutual_at += 1
            turned = []
            for k1 in range(4):
                real = back[k1 * share : (k1 + 1) * share, :quarter]
                imag = back[k1 * share : (k1 + 1) * share, quarter:]
                if k1:
                    cosine, sine = w_ref[k1 : k1 + 1], w_ref[4 + k1 : 5 + k1]
                    real, imag = real * cosine - imag * sine, imag * cosine + real * sine
                turned.append((real, imag))
            s02 = [turned[0][i] + turned[2][i] for i in range(2)]
            d02 = [turned[0][i] - turned[2][i] for i in range(2)]
            s13 = [turned[1][i] + turned[3][i] for i in range(2)]
            d13 = [turned[1][i] - turned[3][i] for i in range(2)]
            real = (s02[0] + s13[0], d02[0] - d13[1], s02[0] - s13[0], d02[0] + d13[1])
            imag = (s02[1] + s13[1], d02[1] + d13[0], s02[1] - s13[1], d02[1] - d13[0])
            lines.append((real, imag))
    width = 4 * quarter // in_ref.shape[0]
    groups = 128 // width
    per_group = len(lines) // groups
    lane = lax.broadcasted_iota(jnp.int32, (share, 128), 1)
    for i in range(per_group):
        for ri in range(2):
            at = (2 * i + ri) * share
            for q in range(4 * quarter // 128):
                j, inside = q * 128 // quarter, q * 128 % quarter
                tiles = [
                    lines[g * per_group + i][ri][j][:, inside : inside + 128]
                    for g in range(groups)
                ]
                for t in range(groups):
                    packed = None
                    for g in range(groups):
                        shift = (g - t) * width % 128
                        tile = pltpu.roll(tiles[g], shift, 1) if shift else tiles[g]
                        packed = tile if g == 0 else jnp.where(lane >= g * width, tile, packed)
                    out_ref[q * groups + t, at : at + share] = packed


def back_kernel(share, in_ref, e_h, e_l, m_h, m_l, o_h, o_l, out_ref):
    devices = in_ref.shape[0]
    groups, per_group, width, length = out_ref.shape
    quarter, eighth = length // 4, length // 8
    for i in range(per_group):
        at = 2 * i * share
        real = in_ref[:, at : at + share].reshape(devices * share, 128).T
        imag = in_ref[:, at + share : at + 2 * share].reshape(devices * share, 128).T

        def both(start, stop):
            return split_value(jnp.concatenate((real[:, start:stop], imag[:, start:stop]), 1))

        even = three_dots(both(0, eighth), (e_h[...], e_l[...]), NN)
        middle = three_dots(both(eighth, quarter), (m_h[...], m_l[...]), NN)
        odd = three_dots(both(quarter, 2 * quarter), (o_h[...], o_l[...]), NN)
        plus, minus = even + middle, even - middle
        first, second = odd[:, :quarter], odd[:, quarter:]
        for j, line in enumerate((plus + first, minus + second, plus - first, minus - second)):
            out_ref[:, i, :, j * quarter : (j + 1) * quarter] = line.reshape(groups, width, quarter)


def swap_kernel(px_count, py_count, in_ref, out_ref, send_sem, recv_sem, own_sem):
    px, py = lax.axis_index("px"), lax.axis_index("py")
    me = px * py_count + py
    count = px_count * py_count
    barrier = pltpu.get_barrier_semaphore()

    def peer(step):
        other_px = lax.rem(px + step // py_count, px_count)
        other_py = lax.rem(py + step % py_count, py_count)
        return other_px, other_py

    for step in range(1, count):
        pl.semaphore_signal(
            barrier, inc=1, device_id=peer(step), device_id_type=pl.DeviceIdType.MESH
        )
    own = pltpu.make_async_copy(in_ref.at[me], out_ref.at[me], own_sem)
    own.start()
    pl.semaphore_wait(barrier, count - 1)
    copies = []
    order = sorted(range(1, count), key=lambda s: -min(s, count - s))
    for step in order:
        other = peer(step)
        copy = pltpu.make_async_remote_copy(
            src_ref=in_ref.at[other[0] * py_count + other[1]],
            dst_ref=out_ref.at[me],
            send_sem=send_sem.at[step],
            recv_sem=recv_sem.at[step],
            device_id=other,
            device_id_type=pl.DeviceIdType.MESH,
        )
        copy.start()
        copies.append(copy)
    own.wait()
    for copy in copies:
        copy.wait()


REMOTE = False


def swap_blocks(value, px_count, py_count, collective):
    if not REMOTE:
        return lax.all_to_all(value, ("px", "py"), split_axis=0, concat_axis=0, tiled=True)
    count = px_count * py_count
    space = pl.BlockSpec(memory_space=pltpu.VMEM)
    return pl.pallas_call(
        functools.partial(swap_kernel, px_count, py_count),
        out_shape=jax.ShapeDtypeStruct(value.shape, value.dtype),
        in_specs=[space],
        out_specs=space,
        scratch_shapes=[
            pltpu.SemaphoreType.DMA((count,)),
            pltpu.SemaphoreType.DMA((count,)),
            pltpu.SemaphoreType.DMA,
        ],
        compiler_params=pltpu.CompilerParams(collective_id=collective, has_side_effects=True),
    )(value)


def register_device(velocity, band_of):
    px_count = lax.axis_size("px")
    py_count = lax.axis_size("py")
    count = px_count * py_count
    _, rows_x, _, span = velocity.shape
    stream = rows_x * px_count
    share = span // 2 // count
    width = stream // count
    groups = 128 // width
    per_group = len(PAIR_LIST) * NB // groups
    vmem = pl.BlockSpec(memory_space=pltpu.VMEM)
    smem = pl.BlockSpec(memory_space=pltpu.SMEM)
    tables = span_tables(span)
    params = pltpu.CompilerParams(vmem_limit_bytes=48 * 1024 * 1024)
    spec = pl.pallas_call(
        functools.partial(span_kernel, share),
        out_shape=jax.ShapeDtypeStruct((count, 3 * share, 128), jnp.float32),
        in_specs=[vmem] * 7,
        out_specs=vmem,
        compiler_params=params,
    )(velocity.reshape(3 * rows_x, span), *tables)
    spec = swap_blocks(spec, px_count, py_count, 0)
    band_ids = lax.iota(jnp.int32, NB)
    onehot = (band_of[:, None] == band_ids[None, :]).astype(jnp.float32)
    cells = float(stream * span)
    weight = onehot / (jnp.sum(onehot, 0)[None, :] * (cells * math.sqrt(cells)))
    me = (lax.axis_index("px") * py_count + lax.axis_index("py")).astype(jnp.int32)
    back = pl.pallas_call(
        functools.partial(stream_kernel, share, py_count),
        out_shape=jax.ShapeDtypeStruct((count, 2 * per_group * share, 128), jnp.float32),
        in_specs=[smem, smem] + [vmem] * 4,
        out_specs=vmem,
        compiler_params=params,
    )(me.reshape(1), weight.reshape(-1), spec, *stream_tables(stream))
    back = swap_blocks(back, px_count, py_count, 1)
    out = pl.pallas_call(
        functools.partial(back_kernel, share),
        out_shape=jax.ShapeDtypeStruct((groups, per_group, width, span), jnp.float32),
        in_specs=[vmem] * 7,
        out_specs=vmem,
        compiler_params=params,
    )(back, *tables)
    return out.reshape(len(PAIR_LIST), NB, width, span)


def fills_registers(velocity, px_count, py_count):
    comps, rows_x, planes, span = velocity.shape
    count = px_count * py_count
    stream = rows_x * px_count
    share = span // 2 // count
    width = max(stream // count, 1)
    return (
        comps == 3
        and rows_x == 64
        and planes == 1
        and px_count % 8 == 0
        and span % 1024 == 0
        and stream % 512 == 0
        and stream == width * count
        and span == 2 * share * count
        and share % 8 == 0
        and 128 % width == 0
        and len(PAIR_LIST) * NB * width % 128 == 0
    )


def per_device(velocity, band_of):
    if fills_registers(velocity, lax.axis_size("px"), lax.axis_size("py")):
        return register_device(velocity, band_of)
    return general_device(velocity, band_of)


def solution(mesh):
    in_specs = (P(None, "px", "py", None), P())
    out_specs = P(None, None, ("px", "py"), None)
    return jax.shard_map(
        per_device, mesh=mesh, in_specs=in_specs, out_specs=out_specs, check_vma=False
    )
```

```python
import functools
import math

import jax
import jax.numpy as jnp
import numpy as np
from jax import lax
from jax.experimental import pallas as pl
from jax.experimental.pallas import tpu as pltpu
from jax.sharding import PartitionSpec as P

NB = 2


PAIR_LIST = ((0, 0), (0, 1), (0, 2), (1, 1), (1, 2), (2, 2))


def phase_table(row_values, offset, count, length):
    col_values = offset + lax.iota(jnp.int32, count)
    phase = row_values[:, None] * col_values[None, :] % length
    angle = phase.astype(jnp.float32) * (2.0 * math.pi / length)
    return (jnp.cos(angle), jnp.sin(angle))


def transform_last(real_part, imag_part, sign):
    full_shape = real_part.shape
    length = full_shape[-1]
    stacked = jnp.concatenate((real_part.reshape(-1, length), imag_part.reshape(-1, length)), 0)
    row_count = stacked.shape[0] // 2
    row_values = lax.iota(jnp.int32, length)

    def one_block(block_index, outputs):
        offset = (block_index * 128).astype(jnp.int32)
        cosine_table, sine_table = phase_table(row_values, offset, 128, length)
        with_cos = jnp.dot(
            stacked,
            cosine_table,
            precision=lax.Precision.HIGHEST,
            preferred_element_type=jnp.float32,
        )
        with_sin = jnp.dot(
            stacked, sine_table, precision=lax.Precision.HIGHEST, preferred_element_type=jnp.float32
        )
        new_real = with_cos[:row_count] - sign * with_sin[row_count:]
        new_imag = with_cos[row_count:] + sign * with_sin[:row_count]
        return (
            lax.dynamic_update_slice_in_dim(outputs[0], new_real, offset, 1),
            lax.dynamic_update_slice_in_dim(outputs[1], new_imag, offset, 1),
        )

    zeros = jnp.zeros((row_count, length), jnp.float32)
    out_real, out_imag = lax.fori_loop(0, length // 128, one_block, (zeros, zeros))
    return (out_real.reshape(full_shape), out_imag.reshape(full_shape))


def span_forward(velocity):
    comps, rows_x, planes, length = velocity.shape
    half = length // 2
    row_values = lax.iota(jnp.int32, length)

    def one_block(block_index, outputs):
        offset = (block_index * 128).astype(jnp.int32)
        cosine_table, sine_table = phase_table(row_values, offset, 128, length)
        with_cos = jnp.einsum(
            "cxpz,zk->cpkx",
            velocity,
            cosine_table,
            precision=lax.Precision.HIGHEST,
            preferred_element_type=jnp.float32,
        )
        with_sin = jnp.einsum(
            "cxpz,zk->cpkx",
            velocity,
            sine_table,
            precision=lax.Precision.HIGHEST,
            preferred_element_type=jnp.float32,
        )
        return (
            lax.dynamic_update_slice_in_dim(outputs[0], with_cos, offset, 2),
            lax.dynamic_update_slice_in_dim(outputs[1], -with_sin, offset, 2),
        )

    zeros = jnp.zeros((comps, planes, half, rows_x), jnp.float32)
    return lax.fori_loop(0, half // 128, one_block, (zeros, zeros))


def span_inverse(summed, kz_order):
    half = summed.shape[3]
    length = 2 * half
    multiplier = jnp.where(kz_order == 0, 1.0, 2.0).astype(jnp.float32)
    held_real = summed[:, :, 0] * multiplier[:, None]
    held_imag = summed[:, :, 1] * multiplier[:, None]

    def one_block(block_index, output):
        offset = (block_index * 128).astype(jnp.int32)
        cosine_table, sine_table = phase_table(kz_order, offset, 128, length)
        part = jnp.einsum(
            "sbkd,kz->sbdz",
            held_real,
            cosine_table,
            precision=lax.Precision.HIGHEST,
            preferred_element_type=jnp.float32,
        )
        part = part - jnp.einsum(
            "sbkd,kz->sbdz",
            held_imag,
            sine_table,
            precision=lax.Precision.HIGHEST,
            preferred_element_type=jnp.float32,
        )
        return lax.dynamic_update_slice_in_dim(output, part, offset, 3)

    zeros = jnp.zeros((summed.shape[0], summed.shape[1], summed.shape[4], length), jnp.float32)
    return lax.fori_loop(0, length // 128, one_block, zeros)


def general_device(velocity, band_of):
    px_count = lax.axis_size("px")
    py_count = lax.axis_size("py")
    comps, rows_x, planes, span = velocity.shape
    stream = rows_x * px_count
    half = span // 2
    local_k = half // px_count
    span_real, span_imag = span_forward(velocity)
    planes_spec = jnp.stack((span_real, span_imag), 1)
    kz_index = lax.iota(jnp.int32, local_k)
    kx_index = lax.iota(jnp.int32, stream)
    at_anchor = jnp.logical_and(
        lax.axis_index("px") == 0, jnp.logical_and(kz_index[:, None] == 0, kx_index[None, :] == 0)
    )
    keep_mask = 1.0 - at_anchor.astype(jnp.float32)
    received = lax.all_to_all(planes_spec, "px", split_axis=3, concat_axis=4, tiled=True)
    front_real, front_imag = transform_last(received[:, 0], received[:, 1], -1.0)
    spectrum = jnp.stack((front_real * keep_mask, front_imag * keep_mask), 1)
    cross_list = []
    for left_comp, right_comp in PAIR_LIST:
        left_real, left_imag = (spectrum[left_comp, 0], spectrum[left_comp, 1])
        right_real, right_imag = (spectrum[right_comp, 0], spectrum[right_comp, 1])
        cross_list.append(
            jnp.stack(
                (
                    left_real * right_real + left_imag * right_imag,
                    left_real * right_imag - left_imag * right_real,
                ),
                0,
            )
        )
    cross = jnp.stack(cross_list, 0)
    band_ids = lax.iota(jnp.int32, NB)
    onehot_all = (band_of[:, None] == band_ids[None, :]).astype(jnp.float32)
    counts = jnp.sum(onehot_all, 0)
    cells = float(stream * span)
    plane_start = lax.axis_index("py") * planes
    local_hot = lax.dynamic_slice_in_dim(onehot_all, plane_start, planes, 0)
    band_weight = local_hot / (counts[None, :] * (cells * math.sqrt(cells)))
    banded = jnp.einsum("sapkx,pb->sbakx", cross, band_weight, precision=lax.Precision.HIGHEST)
    summed = lax.psum_scatter(banded, "py", scatter_dimension=3, tiled=True)
    back_real, back_imag = transform_last(summed[:, :, 0], summed[:, :, 1], 1.0)
    exchanged = lax.all_to_all(
        lax.all_to_all(
            jnp.stack((back_real, back_imag), 2), "px", split_axis=4, concat_axis=3, tiled=True
        ),
        "py",
        split_axis=4,
        concat_axis=3,
        tiled=True,
    )
    quarter = local_k // py_count
    position = lax.iota(jnp.int32, half)
    outer = position // (px_count * quarter)
    remain = position % (px_count * quarter)
    kz_order = remain // quarter * local_k + outer * quarter + remain % quarter
    return span_inverse(exchanged, kz_order)


def split_table(table):
    high = table.astype(jnp.bfloat16)
    low = (table - high.astype(np.float64)).astype(jnp.bfloat16)
    return high, low


def span_tables(length):
    quarter, eighth = length // 4, length // 8
    column = np.arange(quarter)

    def angle(first, count):
        wave = 4 * np.arange(count) + first
        return 2.0 * np.pi * ((wave[:, None] * column[None, :]) % length) / length

    even = angle(0, eighth)
    middle = angle(2, eighth)
    odd = angle(1, quarter)
    table_even = np.concatenate((np.cos(even), -np.sin(even)), 0)
    table_middle = np.concatenate((np.cos(middle), -np.sin(middle)), 0)
    table_odd = np.block([[np.cos(odd), -np.sin(odd)], [-np.sin(odd), -np.cos(odd)]])
    return split_table(table_even) + split_table(table_middle) + split_table(table_odd)


def stream_tables(length):
    quarter = length // 4
    index = np.arange(quarter)
    angle = 2.0 * np.pi * ((index[:, None] * index[None, :]) % quarter) / quarter
    cosine, sine = np.cos(angle), np.sin(angle)
    twist = 2.0 * np.pi * (np.arange(4)[:, None] * index[None, :]) / length
    twiddle = np.concatenate((np.cos(twist), np.sin(twist)), 0).astype(np.float32)
    return split_table(np.block([[cosine, -sine], [sine, cosine]])) + (twiddle,)


def split_value(value):
    high = value.astype(jnp.bfloat16)
    low = (value - high.astype(jnp.float32)).astype(jnp.bfloat16)
    return high, low


def three_dots(left, right, dims):
    def one(a, b):
        return lax.dot_general(a, b, (dims, ((), ())), preferred_element_type=jnp.float32)

    return one(left[0], right[0]) + (one(left[1], right[0]) + one(left[0], right[1]))


NT = ((1,), (1,))
NN = ((1,), (0,))


def span_stage(share, v_ref, e_h, e_l, m_h, m_l, o_h, o_l, out_ref):
    values = v_ref[...]
    rows = values.shape[0] // 3
    values = jnp.concatenate((values, values[2 * rows :]), 0)
    quarter = values.shape[1] // 4
    part = [values[:, i * quarter : (i + 1) * quarter] for i in range(4)]
    plus_even, plus_odd = part[0] + part[2], part[1] + part[3]
    odd_in = jnp.concatenate((part[0] - part[2], part[1] - part[3]), 1)
    even = three_dots((e_h[...], e_l[...]), split_value(plus_even + plus_odd), NT)
    middle = three_dots((m_h[...], m_l[...]), split_value(plus_even - plus_odd), NT)
    odd = three_dots((o_h[...], o_l[...]), split_value(odd_in), NT)
    eighth = quarter // 2
    real = jnp.concatenate((even[:eighth], middle[:eighth], odd[:quarter]), 0)
    imag = jnp.concatenate((even[eighth:], middle[eighth:], odd[quarter:]), 0)
    lane = lax.broadcasted_iota(jnp.int32, (real.shape[0], 128), 1)
    third = jnp.where(lane < 64, real[:, 128:], imag[:, 128:])
    out_ref[:, :share] = real[:, :128].reshape(-1, share, 128)
    out_ref[:, share : 2 * share] = imag[:, :128].reshape(-1, share, 128)
    out_ref[:, 2 * share :] = third.reshape(-1, share, 128)


def stream_stage(share, planes, first_device, band_ref, in_ref, t_h, t_l, w_ref, span_cells, out_ref, send_part):
    px_count = in_ref.shape[0] // planes
    columns = px_count // 2
    group_cols = columns // 4
    quarter = w_ref.shape[1]
    lane = lax.broadcasted_iota(jnp.int32, (3 * share, 128), 1)
    low_half = lane < 64
    cells = []
    for q in range(columns):
        real, imag = [[], [], []], [[], [], []]
        for y in range(planes):
            a = in_ref[2 * q * planes + y]
            b = in_ref[(2 * q + 1) * planes + y]
            low = jnp.where(low_half, a, pltpu.roll(b, 64, 1))
            high = jnp.where(low_half, pltpu.roll(a, 64, 1), b)
            real[0].append(low[:share])
            imag[0].append(low[share : 2 * share])
            real[1].append(high[:share])
            imag[1].append(high[share : 2 * share])
            real[2].append(low[2 * share :])
            imag[2].append(high[2 * share :])
        cells.append(
            (
                jnp.concatenate(real[0] + real[1] + real[2], 0),
                jnp.concatenate(imag[0] + imag[1] + imag[2], 0),
            )
        )
    part = [
        tuple(
            jnp.concatenate([cells[j * group_cols + g][ri] for g in range(group_cols)], 1)
            for ri in range(2)
        )
        for j in range(4)
    ]
    sum02 = [part[0][i] + part[2][i] for i in range(2)]
    dif02 = [part[0][i] - part[2][i] for i in range(2)]
    sum13 = [part[1][i] + part[3][i] for i in range(2)]
    dif13 = [part[1][i] - part[3][i] for i in range(2)]
    mixed = [
        (sum02[0] + sum13[0], sum02[1] + sum13[1]),
        (dif02[0] + dif13[1], dif02[1] - dif13[0]),
        (sum02[0] - sum13[0], sum02[1] - sum13[1]),
        (dif02[0] - dif13[1], dif02[1] + dif13[0]),
    ]
    turned = []
    for k1, (real, imag) in enumerate(mixed):
        if k1:
            cosine, sine = w_ref[k1 : k1 + 1], w_ref[4 + k1 : 5 + k1]
            real, imag = real * cosine + imag * sine, imag * cosine - real * sine
        turned.append(jnp.concatenate((real, imag), 1))
    table = (t_h[...], t_l[...])
    front = three_dots(split_value(jnp.concatenate(turned, 0)), table, NN)
    block = 3 * planes * share
    row = lax.broadcasted_iota(jnp.int32, (block, 2 * quarter), 0)
    col = lax.broadcasted_iota(jnp.int32, (block, 2 * quarter), 1)
    anchor = jnp.logical_and(row % share == 0, col % quarter == 0)
    anchor = jnp.logical_and(anchor, first_device)
    front = jnp.concatenate((jnp.where(anchor, 0.0, front[:block]), front[block:]), 0)
    front = front.reshape(4, 3, planes, share, 2 * quarter)
    field = [
        [
            (
                front[:, c, y, :, :quarter].reshape(4 * share, quarter),
                front[:, c, y, :, quarter:].reshape(4 * share, quarter),
            )
            for y in range(planes)
        ]
        for c in range(3)
    ]
    row = lax.broadcasted_iota(jnp.int32, (4 * share, quarter), 0)
    single = jnp.logical_and(row % share == 0, first_device)
    multiplier = jnp.where(single, 1.0, 2.0)
    onehot, scale = [], []
    for b in range(NB):
        hot = [
            jnp.where(jnp.full((4 * share, quarter), band_ref[y], jnp.int32) == b, 1.0, 0.0)
            for y in range(planes)
        ]
        onehot.append(hot)
        scale.append(multiplier / (sum(hot[1:], hot[0]) * (span_cells * math.sqrt(span_cells))))

    def banded(left, right, b):
        real_sum = imag_sum = None
        for y in range(planes):
            lr, li = field[left][y]
            rr, ri = field[right][y]
            add = onehot[b][y] * (lr * rr + li * ri)
            real_sum = add if y == 0 else real_sum + add
            if left != right:
                add = onehot[b][y] * (lr * ri - li * rr)
                imag_sum = add if y == 0 else imag_sum + add
        if left == right:
            return real_sum * scale[b]
        return jnp.concatenate((real_sum * scale[b], imag_sum * scale[b]), 1)

    own_table = (t_h[:, :quarter], t_l[:, :quarter])

    def lines_of(members):
        value = [banded(*PAIR_LIST[m // NB], m % NB) for m in members]
        result = [None] * len(members)
        for columns_in, used in ((quarter, own_table), (2 * quarter, table)):
            chosen = [n for n in range(len(members)) if value[n].shape[1] == columns_in]
            if not chosen:
                continue
            joined = jnp.concatenate([value[n] for n in chosen], 0)
            whole = three_dots(split_value(joined), used, NT)
            for place, n in enumerate(chosen):
                result[n] = spread(whole[place * 4 * share : (place + 1) * 4 * share])
        return result

    def spread(back):
        turned = []
        for k1 in range(4):
            real = back[k1 * share : (k1 + 1) * share, :quarter]
            imag = back[k1 * share : (k1 + 1) * share, quarter:]
            if k1:
                cosine, sine = w_ref[k1 : k1 + 1], w_ref[4 + k1 : 5 + k1]
                real, imag = real * cosine - imag * sine, imag * cosine + real * sine
            turned.append((real, imag))
        s02 = [turned[0][i] + turned[2][i] for i in range(2)]
        d02 = [turned[0][i] - turned[2][i] for i in range(2)]
        s13 = [turned[1][i] + turned[3][i] for i in range(2)]
        d13 = [turned[1][i] - turned[3][i] for i in range(2)]
        real = (s02[0] + s13[0], d02[0] - d13[1], s02[0] - s13[0], d02[0] + d13[1])
        imag = (s02[1] + s13[1], d02[1] + d13[0], s02[1] - s13[1], d02[1] - d13[0])
        return real, imag

    width = 4 * quarter // in_ref.shape[0]
    groups = 128 // width
    per_group = out_ref.shape[0]
    lane = lax.broadcasted_iota(jnp.int32, (share, 128), 1)
    for i in range(per_group):
        lines = lines_of([g * per_group + i for g in range(groups)])
        for ri in range(2):
            at = ri * share
            for q in range(4 * quarter // 128):
                j, inside = q * 128 // quarter, q * 128 % quarter
                tiles = [lines[g][ri][j][:, inside : inside + 128] for g in range(groups)]
                for t in range(groups):
                    packed = None
                    for g in range(groups):
                        shift = (g - t) * width % 128
                        tile = pltpu.roll(tiles[g], shift, 1) if shift else tiles[g]
                        packed = tile if g == 0 else jnp.where(lane >= g * width, tile, packed)
                    out_ref[i, q * groups + t, at : at + share] = packed
        send_part(i)


def back_stage(share, i, in_ref, e_h, e_l, m_h, m_l, o_h, o_l, out_ref):
    devices = in_ref.shape[1]
    _, groups, width, length = out_ref.shape
    quarter, eighth = length // 4, length // 8
    real = in_ref[i, :, :share].reshape(devices * share, 128).T
    imag = in_ref[i, :, share : 2 * share].reshape(devices * share, 128).T

    def both(start, stop):
        return split_value(jnp.concatenate((real[:, start:stop], imag[:, start:stop]), 1))

    even = three_dots(both(0, eighth), (e_h[...], e_l[...]), NN)
    middle = three_dots(both(eighth, quarter), (m_h[...], m_l[...]), NN)
    odd = three_dots(both(quarter, 2 * quarter), (o_h[...], o_l[...]), NN)
    plus, minus = even + middle, even - middle
    first, second = odd[:, :quarter], odd[:, quarter:]
    for j, line in enumerate((plus + first, minus + second, plus - first, minus - second)):
        out_ref[i, :, :, j * quarter : (j + 1) * quarter] = line.reshape(groups, width, quarter)


def flip_bits(index, bits):
    moved, bit = index, 1
    while bit <= bits:
        if bits & bit:
            moved = moved + bit * (1 - 2 * ((index // bit) % 2))
        bit *= 2
    return moved


def whole_kernel(
    px_count,
    py_count,
    share,
    band_ref,
    v_far,
    e_h_far,
    e_l_far,
    m_h_far,
    m_l_far,
    o_h_far,
    o_l_far,
    t_h_far,
    t_l_far,
    w_far,
    out_ref,
    v_ref,
    e_h,
    e_l,
    m_h,
    m_l,
    o_h,
    o_l,
    t_h,
    t_l,
    w_ref,
    spec_out,
    spec_in,
    back_out,
    back_in,
    result,
    send_sem,
    recv_sem,
    own_sem,
    table_sem,
    out_sem,
):
    far = (v_far, o_h_far, o_l_far, e_h_far, e_l_far, m_h_far, m_l_far)
    near = (v_ref, o_h, o_l, e_h, e_l, m_h, m_l)
    far, near = far + (t_h_far, t_l_far, w_far), near + (t_h, t_l, w_ref)
    loads = [
        pltpu.make_async_copy(far[n], near[n], table_sem.at[n]) for n in range(len(far))
    ]
    for load in loads:
        load.start()
    px, py = lax.axis_index("px"), lax.axis_index("py")
    me = px * py_count + py
    count = px_count * py_count
    parts = back_out.shape[0]
    barrier = pltpu.get_barrier_semaphore()
    steps = list(range(count - 1, 0, -1))
    peers = {s: (flip_bits(px, s // py_count), flip_bits(py, s % py_count)) for s in steps}
    for s in steps:
        pl.semaphore_signal(
            barrier, inc=1, device_id=peers[s], device_id_type=pl.DeviceIdType.MESH
        )
    def swap(lane, source, target):
        own = pltpu.make_async_copy(source.at[me], target.at[me], own_sem.at[lane])
        copies = []
        for s in steps:
            copy = pltpu.make_async_remote_copy(
                src_ref=source.at[peers[s][0] * py_count + peers[s][1]],
                dst_ref=target.at[me],
                send_sem=send_sem.at[lane, s],
                recv_sem=recv_sem.at[lane, s],
                device_id=peers[s],
                device_id_type=pl.DeviceIdType.MESH,
            )
            copy.start()
            copies.append(copy)
        own.start()
        return own, copies

    def arrive(moves):
        moves[0].wait()
        for copy in moves[1]:
            copy.wait_recv()

    for load in loads[:7]:
        load.wait()
    span_stage(share, v_ref, e_h, e_l, m_h, m_l, o_h, o_l, spec_out)
    pl.semaphore_wait(barrier, count - 1)
    moves = [swap(0, spec_out, spec_in)]
    for load in loads[7:]:
        load.wait()
    arrive(moves[0])

    def send_part(i):
        moves.append(swap(1 + i, back_out.at[i], back_in.at[i]))

    cells = float(v_ref.shape[1] * 4 * w_ref.shape[1])
    stream_stage(
        share, py_count, me == 0, band_ref, spec_in, t_h, t_l, w_ref, cells, back_out, send_part
    )
    stores = []
    for i in range(parts):
        arrive(moves[1 + i])
        back_stage(share, i, back_in, e_h, e_l, m_h, m_l, o_h, o_l, result)
        store = pltpu.make_async_copy(result.at[i], out_ref.at[:, i], out_sem.at[i])
        store.start()
        stores.append(store)
    for _, copies in moves:
        for copy in copies:
            copy.wait_send()
    for store in stores:
        store.wait()


def register_device(velocity, band_of):
    px_count = lax.axis_size("px")
    py_count = lax.axis_size("py")
    count = px_count * py_count
    _, rows_x, _, span = velocity.shape
    stream = rows_x * px_count
    share = span // 2 // count
    width = stream // count
    groups = 128 // width
    parts = len(PAIR_LIST) * NB // groups
    smem = pl.BlockSpec(memory_space=pltpu.SMEM)
    far = pl.BlockSpec(memory_space=pl.ANY)
    spec_shape = (count, 3 * share, 128)
    back_shape = (parts, count, 2 * share, 128)
    operands = (velocity.reshape(3 * rows_x, span),) + span_tables(span) + stream_tables(stream)
    out = pl.pallas_call(
        functools.partial(whole_kernel, px_count, py_count, share),
        out_shape=jax.ShapeDtypeStruct((groups, parts, width, span), jnp.float32),
        in_specs=[smem] + [far] * len(operands),
        out_specs=far,
        scratch_shapes=[pltpu.VMEM(x.shape, x.dtype) for x in operands]
        + [
            pltpu.VMEM(spec_shape, jnp.float32),
            pltpu.VMEM(spec_shape, jnp.float32),
            pltpu.VMEM(back_shape, jnp.float32),
            pltpu.VMEM(back_shape, jnp.float32),
            pltpu.VMEM((parts, groups, width, span), jnp.float32),
            pltpu.SemaphoreType.DMA((1 + parts, count)),
            pltpu.SemaphoreType.DMA((1 + parts, count)),
            pltpu.SemaphoreType.DMA((1 + parts,)),
            pltpu.SemaphoreType.DMA((len(operands),)),
            pltpu.SemaphoreType.DMA((parts,)),
        ],
        compiler_params=pltpu.CompilerParams(
            collective_id=0, has_side_effects=True, vmem_limit_bytes=60 * 1024 * 1024
        ),
    )(band_of, *operands)
    return out.reshape(len(PAIR_LIST), NB, width, span)


def fills_registers(velocity, px_count, py_count):
    comps, rows_x, planes, span = velocity.shape
    count = px_count * py_count
    stream = rows_x * px_count
    share = span // 2 // count
    width = max(stream // count, 1)
    return (
        comps == 3
        and rows_x == 64
        and planes == 1
        and px_count & (px_count - 1) == 0
        and py_count & (py_count - 1) == 0
        and px_count % 8 == 0
        and span % 1024 == 0
        and stream % 512 == 0
        and stream == width * count
        and span == 2 * share * count
        and share % 8 == 0
        and 128 % width == 0
        and len(PAIR_LIST) * NB * width % 128 == 0
    )


def per_device(velocity, band_of):
    if fills_registers(velocity, lax.axis_size("px"), lax.axis_size("py")):
        return register_device(velocity, band_of)
    return general_device(velocity, band_of)


def solution(mesh):
    in_specs = (P(None, "px", "py", None), P())
    out_specs = P(None, None, ("px", "py"), None)
    return jax.shard_map(
        per_device, mesh=mesh, in_specs=in_specs, out_specs=out_specs, check_vma=False
    )
```

```python
import functools
import math

import jax
import jax.numpy as jnp
import numpy as np
from jax import lax
from jax.experimental import pallas as pl
from jax.experimental.pallas import tpu as pltpu
from jax.sharding import PartitionSpec as P

NB = 2


PAIR_LIST = ((0, 0), (0, 1), (0, 2), (1, 1), (1, 2), (2, 2))


def phase_table(row_values, offset, count, length):
    col_values = offset + lax.iota(jnp.int32, count)
    phase = row_values[:, None] * col_values[None, :] % length
    angle = phase.astype(jnp.float32) * (2.0 * math.pi / length)
    return (jnp.cos(angle), jnp.sin(angle))


def transform_last(real_part, imag_part, sign):
    full_shape = real_part.shape
    length = full_shape[-1]
    stacked = jnp.concatenate((real_part.reshape(-1, length), imag_part.reshape(-1, length)), 0)
    row_count = stacked.shape[0] // 2
    row_values = lax.iota(jnp.int32, length)

    def one_block(block_index, outputs):
        offset = (block_index * 128).astype(jnp.int32)
        cosine_table, sine_table = phase_table(row_values, offset, 128, length)
        with_cos = jnp.dot(
            stacked,
            cosine_table,
            precision=lax.Precision.HIGHEST,
            preferred_element_type=jnp.float32,
        )
        with_sin = jnp.dot(
            stacked, sine_table, precision=lax.Precision.HIGHEST, preferred_element_type=jnp.float32
        )
        new_real = with_cos[:row_count] - sign * with_sin[row_count:]
        new_imag = with_cos[row_count:] + sign * with_sin[:row_count]
        return (
            lax.dynamic_update_slice_in_dim(outputs[0], new_real, offset, 1),
            lax.dynamic_update_slice_in_dim(outputs[1], new_imag, offset, 1),
        )

    zeros = jnp.zeros((row_count, length), jnp.float32)
    out_real, out_imag = lax.fori_loop(0, length // 128, one_block, (zeros, zeros))
    return (out_real.reshape(full_shape), out_imag.reshape(full_shape))


def span_forward(velocity):
    comps, rows_x, planes, length = velocity.shape
    half = length // 2
    row_values = lax.iota(jnp.int32, length)

    def one_block(block_index, outputs):
        offset = (block_index * 128).astype(jnp.int32)
        cosine_table, sine_table = phase_table(row_values, offset, 128, length)
        with_cos = jnp.einsum(
            "cxpz,zk->cpkx",
            velocity,
            cosine_table,
            precision=lax.Precision.HIGHEST,
            preferred_element_type=jnp.float32,
        )
        with_sin = jnp.einsum(
            "cxpz,zk->cpkx",
            velocity,
            sine_table,
            precision=lax.Precision.HIGHEST,
            preferred_element_type=jnp.float32,
        )
        return (
            lax.dynamic_update_slice_in_dim(outputs[0], with_cos, offset, 2),
            lax.dynamic_update_slice_in_dim(outputs[1], -with_sin, offset, 2),
        )

    zeros = jnp.zeros((comps, planes, half, rows_x), jnp.float32)
    return lax.fori_loop(0, half // 128, one_block, (zeros, zeros))


def span_inverse(summed, kz_order):
    half = summed.shape[3]
    length = 2 * half
    multiplier = jnp.where(kz_order == 0, 1.0, 2.0).astype(jnp.float32)
    held_real = summed[:, :, 0] * multiplier[:, None]
    held_imag = summed[:, :, 1] * multiplier[:, None]

    def one_block(block_index, output):
        offset = (block_index * 128).astype(jnp.int32)
        cosine_table, sine_table = phase_table(kz_order, offset, 128, length)
        part = jnp.einsum(
            "sbkd,kz->sbdz",
            held_real,
            cosine_table,
            precision=lax.Precision.HIGHEST,
            preferred_element_type=jnp.float32,
        )
        part = part - jnp.einsum(
            "sbkd,kz->sbdz",
            held_imag,
            sine_table,
            precision=lax.Precision.HIGHEST,
            preferred_element_type=jnp.float32,
        )
        return lax.dynamic_update_slice_in_dim(output, part, offset, 3)

    zeros = jnp.zeros((summed.shape[0], summed.shape[1], summed.shape[4], length), jnp.float32)
    return lax.fori_loop(0, length // 128, one_block, zeros)


def general_device(velocity, band_of):
    px_count = lax.axis_size("px")
    py_count = lax.axis_size("py")
    comps, rows_x, planes, span = velocity.shape
    stream = rows_x * px_count
    half = span // 2
    local_k = half // px_count
    span_real, span_imag = span_forward(velocity)
    planes_spec = jnp.stack((span_real, span_imag), 1)
    kz_index = lax.iota(jnp.int32, local_k)
    kx_index = lax.iota(jnp.int32, stream)
    at_anchor = jnp.logical_and(
        lax.axis_index("px") == 0, jnp.logical_and(kz_index[:, None] == 0, kx_index[None, :] == 0)
    )
    keep_mask = 1.0 - at_anchor.astype(jnp.float32)
    received = lax.all_to_all(planes_spec, "px", split_axis=3, concat_axis=4, tiled=True)
    front_real, front_imag = transform_last(received[:, 0], received[:, 1], -1.0)
    spectrum = jnp.stack((front_real * keep_mask, front_imag * keep_mask), 1)
    cross_list = []
    for left_comp, right_comp in PAIR_LIST:
        left_real, left_imag = (spectrum[left_comp, 0], spectrum[left_comp, 1])
        right_real, right_imag = (spectrum[right_comp, 0], spectrum[right_comp, 1])
        cross_list.append(
            jnp.stack(
                (
                    left_real * right_real + left_imag * right_imag,
                    left_real * right_imag - left_imag * right_real,
                ),
                0,
            )
        )
    cross = jnp.stack(cross_list, 0)
    band_ids = lax.iota(jnp.int32, NB)
    onehot_all = (band_of[:, None] == band_ids[None, :]).astype(jnp.float32)
    counts = jnp.sum(onehot_all, 0)
    cells = float(stream * span)
    plane_start = lax.axis_index("py") * planes
    local_hot = lax.dynamic_slice_in_dim(onehot_all, plane_start, planes, 0)
    band_weight = local_hot / (counts[None, :] * (cells * math.sqrt(cells)))
    banded = jnp.einsum("sapkx,pb->sbakx", cross, band_weight, precision=lax.Precision.HIGHEST)
    summed = lax.psum_scatter(banded, "py", scatter_dimension=3, tiled=True)
    back_real, back_imag = transform_last(summed[:, :, 0], summed[:, :, 1], 1.0)
    exchanged = lax.all_to_all(
        lax.all_to_all(
            jnp.stack((back_real, back_imag), 2), "px", split_axis=4, concat_axis=3, tiled=True
        ),
        "py",
        split_axis=4,
        concat_axis=3,
        tiled=True,
    )
    quarter = local_k // py_count
    position = lax.iota(jnp.int32, half)
    outer = position // (px_count * quarter)
    remain = position % (px_count * quarter)
    kz_order = remain // quarter * local_k + outer * quarter + remain % quarter
    return span_inverse(exchanged, kz_order)


def split_table(table):
    high = table.astype(jnp.bfloat16)
    low = (table - high.astype(np.float64)).astype(jnp.bfloat16)
    return high, low


def span_tables(length):
    quarter, eighth = length // 4, length // 8
    column = np.arange(quarter)

    def angle(first, count):
        wave = 4 * np.arange(count) + first
        return 2.0 * np.pi * ((wave[:, None] * column[None, :]) % length) / length

    even = angle(0, eighth)
    middle = angle(2, eighth)
    odd = angle(1, quarter)
    table_even = np.concatenate((np.cos(even), -np.sin(even)), 0)
    table_middle = np.concatenate((np.cos(middle), -np.sin(middle)), 0)
    table_odd = np.block([[np.cos(odd), -np.sin(odd)], [-np.sin(odd), -np.cos(odd)]])
    return split_table(table_even) + split_table(table_middle) + split_table(table_odd)


def stream_tables(length):
    quarter = length // 4
    index = np.arange(quarter)
    angle = 2.0 * np.pi * ((index[:, None] * index[None, :]) % quarter) / quarter
    cosine, sine = np.cos(angle), np.sin(angle)
    twist = 2.0 * np.pi * (np.arange(4)[:, None] * index[None, :]) / length
    twiddle = np.concatenate((np.cos(twist), np.sin(twist)), 0).astype(np.float32)
    return split_table(np.block([[cosine, -sine], [sine, cosine]])) + (twiddle,)


def split_value(value):
    high = value.astype(jnp.bfloat16)
    low = (value - high.astype(jnp.float32)).astype(jnp.bfloat16)
    return high, low


def three_dots(left, right, dims):
    def one(a, b):
        return lax.dot_general(a, b, (dims, ((), ())), preferred_element_type=jnp.float32)

    return one(left[0], right[0]) + (one(left[1], right[0]) + one(left[0], right[1]))


NT = ((1,), (1,))
NN = ((1,), (0,))


def span_stage(share, v_ref, e_h, e_l, m_h, m_l, o_h, o_l, out_ref):
    values = v_ref[...]
    rows = values.shape[0] // 3
    values = jnp.concatenate((values, values[2 * rows :]), 0)
    quarter = values.shape[1] // 4
    part = [values[:, i * quarter : (i + 1) * quarter] for i in range(4)]
    plus_even, plus_odd = part[0] + part[2], part[1] + part[3]
    odd_in = jnp.concatenate((part[0] - part[2], part[1] - part[3]), 1)
    even = three_dots((e_h[...], e_l[...]), split_value(plus_even + plus_odd), NT)
    middle = three_dots((m_h[...], m_l[...]), split_value(plus_even - plus_odd), NT)
    odd = three_dots((o_h[...], o_l[...]), split_value(odd_in), NT)
    eighth = quarter // 2
    real = jnp.concatenate((even[:eighth], middle[:eighth], odd[:quarter]), 0)
    imag = jnp.concatenate((even[eighth:], middle[eighth:], odd[quarter:]), 0)
    lane = lax.broadcasted_iota(jnp.int32, (real.shape[0], 128), 1)
    third = jnp.where(lane < 64, real[:, 128:], imag[:, 128:])
    out_ref[:, :share] = real[:, :128].reshape(-1, share, 128)
    out_ref[:, share : 2 * share] = imag[:, :128].reshape(-1, share, 128)
    out_ref[:, 2 * share :] = third.reshape(-1, share, 128)


def stream_stage(share, planes, first_device, band_ref, in_ref, t_h, t_l, w_ref, span_cells, out_ref, send_part):
    px_count = in_ref.shape[0] // planes
    columns = px_count // 2
    group_cols = columns // 4
    quarter = w_ref.shape[1]
    lane = lax.broadcasted_iota(jnp.int32, (3 * share, 128), 1)
    low_half = lane < 64
    cells = []
    for q in range(columns):
        real, imag = [[], [], []], [[], [], []]
        for y in range(planes):
            a = in_ref[2 * q * planes + y]
            b = in_ref[(2 * q + 1) * planes + y]
            low = jnp.where(low_half, a, pltpu.roll(b, 64, 1))
            high = jnp.where(low_half, pltpu.roll(a, 64, 1), b)
            real[0].append(low[:share])
            imag[0].append(low[share : 2 * share])
            real[1].append(high[:share])
            imag[1].append(high[share : 2 * share])
            real[2].append(low[2 * share :])
            imag[2].append(high[2 * share :])
        cells.append(
            (
                jnp.concatenate(real[0] + real[1] + real[2], 0),
                jnp.concatenate(imag[0] + imag[1] + imag[2], 0),
            )
        )
    part = [
        tuple(
            jnp.concatenate([cells[j * group_cols + g][ri] for g in range(group_cols)], 1)
            for ri in range(2)
        )
        for j in range(4)
    ]
    sum02 = [part[0][i] + part[2][i] for i in range(2)]
    dif02 = [part[0][i] - part[2][i] for i in range(2)]
    sum13 = [part[1][i] + part[3][i] for i in range(2)]
    dif13 = [part[1][i] - part[3][i] for i in range(2)]
    mixed = [
        (sum02[0] + sum13[0], sum02[1] + sum13[1]),
        (dif02[0] + dif13[1], dif02[1] - dif13[0]),
        (sum02[0] - sum13[0], sum02[1] - sum13[1]),
        (dif02[0] - dif13[1], dif02[1] + dif13[0]),
    ]
    turned = []
    for k1, (real, imag) in enumerate(mixed):
        if k1:
            cosine, sine = w_ref[k1 : k1 + 1], w_ref[4 + k1 : 5 + k1]
            real, imag = real * cosine + imag * sine, imag * cosine - real * sine
        turned.append(jnp.concatenate((real, imag), 1))
    table = (t_h[...], t_l[...])
    front = three_dots(split_value(jnp.concatenate(turned, 0)), table, NN)
    block = 3 * planes * share
    row = lax.broadcasted_iota(jnp.int32, (block, 2 * quarter), 0)
    col = lax.broadcasted_iota(jnp.int32, (block, 2 * quarter), 1)
    anchor = jnp.logical_and(row % share == 0, col % quarter == 0)
    anchor = jnp.logical_and(anchor, first_device)
    front = jnp.concatenate((jnp.where(anchor, 0.0, front[:block]), front[block:]), 0)
    front = front.reshape(4, 3, planes, share, 2 * quarter)
    field = [
        [
            (
                front[:, c, y, :, :quarter].reshape(4 * share, quarter),
                front[:, c, y, :, quarter:].reshape(4 * share, quarter),
            )
            for y in range(planes)
        ]
        for c in range(3)
    ]
    row = lax.broadcasted_iota(jnp.int32, (4 * share, quarter), 0)
    single = jnp.logical_and(row % share == 0, first_device)
    multiplier = jnp.where(single, 1.0, 2.0)
    onehot, scale = [], []
    for b in range(NB):
        hot = [
            jnp.where(jnp.full((4 * share, quarter), band_ref[y], jnp.int32) == b, 1.0, 0.0)
            for y in range(planes)
        ]
        onehot.append(hot)
        scale.append(multiplier / (sum(hot[1:], hot[0]) * (span_cells * math.sqrt(span_cells))))

    def banded(left, right, b):
        real_sum = imag_sum = None
        for y in range(planes):
            lr, li = field[left][y]
            rr, ri = field[right][y]
            add = onehot[b][y] * (lr * rr + li * ri)
            real_sum = add if y == 0 else real_sum + add
            if left != right:
                add = onehot[b][y] * (lr * ri - li * rr)
                imag_sum = add if y == 0 else imag_sum + add
        if left == right:
            return real_sum * scale[b]
        return jnp.concatenate((real_sum * scale[b], imag_sum * scale[b]), 1)

    own_table = (t_h[:, :quarter], t_l[:, :quarter])

    def lines_of(members):
        value = [banded(*PAIR_LIST[m // NB], m % NB) for m in members]
        result = [None] * len(members)
        for columns_in, used in ((quarter, own_table), (2 * quarter, table)):
            chosen = [n for n in range(len(members)) if value[n].shape[1] == columns_in]
            if not chosen:
                continue
            joined = jnp.concatenate([value[n] for n in chosen], 0)
            whole = three_dots(split_value(joined), used, NT)
            for place, n in enumerate(chosen):
                result[n] = spread(whole[place * 4 * share : (place + 1) * 4 * share])
        return result

    def spread(back):
        turned = []
        for k1 in range(4):
            real = back[k1 * share : (k1 + 1) * share, :quarter]
            imag = back[k1 * share : (k1 + 1) * share, quarter:]
            if k1:
                cosine, sine = w_ref[k1 : k1 + 1], w_ref[4 + k1 : 5 + k1]
                real, imag = real * cosine - imag * sine, imag * cosine + real * sine
            turned.append((real, imag))
        s02 = [turned[0][i] + turned[2][i] for i in range(2)]
        d02 = [turned[0][i] - turned[2][i] for i in range(2)]
        s13 = [turned[1][i] + turned[3][i] for i in range(2)]
        d13 = [turned[1][i] - turned[3][i] for i in range(2)]
        real = (s02[0] + s13[0], d02[0] - d13[1], s02[0] - s13[0], d02[0] + d13[1])
        imag = (s02[1] + s13[1], d02[1] + d13[0], s02[1] - s13[1], d02[1] - d13[0])
        return real, imag

    width = 4 * quarter // in_ref.shape[0]
    groups = 128 // width
    per_group = out_ref.shape[0]
    lane = lax.broadcasted_iota(jnp.int32, (share, 128), 1)
    for i in range(per_group):
        lines = lines_of([g * per_group + i for g in range(groups)])
        for ri in range(2):
            at = ri * share
            for q in range(4 * quarter // 128):
                j, inside = q * 128 // quarter, q * 128 % quarter
                tiles = [lines[g][ri][j][:, inside : inside + 128] for g in range(groups)]
                for t in range(groups):
                    packed = None
                    for g in range(groups):
                        shift = (g - t) * width % 128
                        tile = pltpu.roll(tiles[g], shift, 1) if shift else tiles[g]
                        packed = tile if g == 0 else jnp.where(lane >= g * width, tile, packed)
                    out_ref[i, q * groups + t, at : at + share] = packed
        send_part(i)


def back_stage(share, i, in_ref, e_h, e_l, m_h, m_l, o_h, o_l, out_ref):
    devices = in_ref.shape[1]
    _, groups, width, length = out_ref.shape
    quarter, eighth = length // 4, length // 8
    real = in_ref[i, :, :share].reshape(devices * share, 128).T
    imag = in_ref[i, :, share : 2 * share].reshape(devices * share, 128).T

    def both(start, stop):
        return split_value(jnp.concatenate((real[:, start:stop], imag[:, start:stop]), 1))

    even = three_dots(both(0, eighth), (e_h[...], e_l[...]), NN)
    middle = three_dots(both(eighth, quarter), (m_h[...], m_l[...]), NN)
    odd = three_dots(both(quarter, 2 * quarter), (o_h[...], o_l[...]), NN)
    plus, minus = even + middle, even - middle
    first, second = odd[:, :quarter], odd[:, quarter:]
    for j, line in enumerate((plus + first, minus + second, plus - first, minus - second)):
        out_ref[i, :, :, j * quarter : (j + 1) * quarter] = line.reshape(groups, width, quarter)


def flip_bits(index, bits):
    moved, bit = index, 1
    while bit <= bits:
        if bits & bit:
            moved = moved + bit * (1 - 2 * ((index // bit) % 2))
        bit *= 2
    return moved


def whole_kernel(
    px_count,
    py_count,
    share,
    band_ref,
    v_ref,
    table_far,
    w_ref,
    out_ref,
    tables,
    spec_out,
    spec_in,
    back_out,
    back_in,
    result,
    send_sem,
    recv_sem,
    own_sem,
    table_sem,
    out_sem,
):
    quarter = v_ref.shape[1] // 4
    cuts = (0, 2 * quarter, 6 * quarter, 8 * quarter, 10 * quarter)
    loads = [
        pltpu.make_async_copy(
            table_far.at[start:stop], tables.at[start:stop], table_sem.at[n]
        )
        for n, (start, stop) in enumerate(zip(cuts[:-1], cuts[1:]))
    ]
    e_h, m_h = tables.at[:quarter, :quarter], tables.at[:quarter, quarter:]
    e_l = tables.at[quarter : 2 * quarter, :quarter]
    m_l = tables.at[quarter : 2 * quarter, quarter:]
    o_h = tables.at[2 * quarter : 4 * quarter]
    o_l = tables.at[4 * quarter : 6 * quarter]
    t_h = tables.at[6 * quarter : 8 * quarter]
    t_l = tables.at[8 * quarter :]
    for load in loads:
        load.start()
    px, py = lax.axis_index("px"), lax.axis_index("py")
    me = px * py_count + py
    count = px_count * py_count
    parts = back_out.shape[0]
    barrier = pltpu.get_barrier_semaphore()
    steps = list(range(count - 1, 0, -1))
    peers = {s: (flip_bits(px, s // py_count), flip_bits(py, s % py_count)) for s in steps}
    for s in steps:
        pl.semaphore_signal(
            barrier, inc=1, device_id=peers[s], device_id_type=pl.DeviceIdType.MESH
        )
    def swap(lane, source, target):
        own = pltpu.make_async_copy(source.at[me], target.at[me], own_sem.at[lane])
        copies = []
        for s in steps:
            copy = pltpu.make_async_remote_copy(
                src_ref=source.at[peers[s][0] * py_count + peers[s][1]],
                dst_ref=target.at[me],
                send_sem=send_sem.at[lane, s],
                recv_sem=recv_sem.at[lane, s],
                device_id=peers[s],
                device_id_type=pl.DeviceIdType.MESH,
            )
            copy.start()
            copies.append(copy)
        own.start()
        return own, copies

    def arrive(moves):
        moves[0].wait()
        for copy in moves[1]:
            copy.wait_recv()

    for load in loads[:2]:
        load.wait()
    span_stage(share, v_ref, e_h, e_l, m_h, m_l, o_h, o_l, spec_out)
    pl.semaphore_wait(barrier, count - 1)
    moves = [swap(0, spec_out, spec_in)]
    for load in loads[2:]:
        load.wait()
    arrive(moves[0])

    def send_part(i):
        moves.append(swap(1 + i, back_out.at[i], back_in.at[i]))

    cells = float(v_ref.shape[1] * 4 * w_ref.shape[1])
    stream_stage(
        share, py_count, me == 0, band_ref, spec_in, t_h, t_l, w_ref, cells, back_out, send_part
    )
    stores = []
    for i in range(parts):
        arrive(moves[1 + i])
        back_stage(share, i, back_in, e_h, e_l, m_h, m_l, o_h, o_l, result)
        store = pltpu.make_async_copy(result.at[i], out_ref.at[:, i], out_sem.at[i])
        store.start()
        stores.append(store)
    for _, copies in moves:
        for copy in copies:
            copy.wait_send()
    for store in stores:
        store.wait()


def register_device(velocity, band_of):
    px_count = lax.axis_size("px")
    py_count = lax.axis_size("py")
    count = px_count * py_count
    _, rows_x, _, span = velocity.shape
    stream = rows_x * px_count
    share = span // 2 // count
    width = stream // count
    groups = 128 // width
    parts = len(PAIR_LIST) * NB // groups
    vmem = pl.BlockSpec(memory_space=pltpu.VMEM)
    smem = pl.BlockSpec(memory_space=pltpu.SMEM)
    far = pl.BlockSpec(memory_space=pl.ANY)
    spec_shape = (count, 3 * share, 128)
    back_shape = (parts, count, 2 * share, 128)
    e_h, e_l, m_h, m_l, o_h, o_l = span_tables(span)
    t_h, t_l, twiddle = stream_tables(stream)
    even = [np.concatenate(pair, 1) for pair in ((e_h, m_h), (e_l, m_l))]
    tables = np.concatenate(even + [o_h, o_l, t_h, t_l], 0)
    out = pl.pallas_call(
        functools.partial(whole_kernel, px_count, py_count, share),
        out_shape=jax.ShapeDtypeStruct((groups, parts, width, span), jnp.float32),
        in_specs=[smem, vmem, far, vmem],
        out_specs=far,
        scratch_shapes=[
            pltpu.VMEM(tables.shape, tables.dtype),
            pltpu.VMEM(spec_shape, jnp.float32),
            pltpu.VMEM(spec_shape, jnp.float32),
            pltpu.VMEM(back_shape, jnp.float32),
            pltpu.VMEM(back_shape, jnp.float32),
            pltpu.VMEM((parts, groups, width, span), jnp.float32),
            pltpu.SemaphoreType.DMA((1 + parts, count)),
            pltpu.SemaphoreType.DMA((1 + parts, count)),
            pltpu.SemaphoreType.DMA((1 + parts,)),
            pltpu.SemaphoreType.DMA((4,)),
            pltpu.SemaphoreType.DMA((parts,)),
        ],
        compiler_params=pltpu.CompilerParams(
            collective_id=0, has_side_effects=True, vmem_limit_bytes=49152 * 1024
        ),
    )(band_of, velocity.reshape(3 * rows_x, span), tables, twiddle)
    return out.reshape(len(PAIR_LIST), NB, width, span)


def fills_registers(velocity, px_count, py_count):
    comps, rows_x, planes, span = velocity.shape
    count = px_count * py_count
    stream = rows_x * px_count
    share = span // 2 // count
    width = max(stream // count, 1)
    return (
        comps == 3
        and rows_x == 64
        and planes == 1
        and px_count & (px_count - 1) == 0
        and py_count & (py_count - 1) == 0
        and px_count % 8 == 0
        and span % 1024 == 0
        and stream == span
        and stream == width * count
        and span == 2 * share * count
        and share % 8 == 0
        and 128 % width == 0
        and len(PAIR_LIST) * NB * width % 128 == 0
    )


def per_device(velocity, band_of):
    if fills_registers(velocity, lax.axis_size("px"), lax.axis_size("py")):
        return register_device(velocity, band_of)
    return general_device(velocity, band_of)


def solution(mesh):
    in_specs = (P(None, "px", "py", None), P())
    out_specs = P(None, None, ("px", "py"), None)
    return jax.shard_map(
        per_device, mesh=mesh, in_specs=in_specs, out_specs=out_specs, check_vma=False
    )
```
